256 devices in a mesh: lon: 16 (over y_hi, z), day: 16 (over x, y_lo, core).
Axes of the slice: x: 4, y: 4 (y_hi: 2, y_lo: 2; y = y_hi * 2 + y_lo), z: 8, core: 2. Of those that a mesh axis runs over, the one named last changes fastest.
Arguments:
- field: bfloat16 [368, 1440, 1024], P('day', 'lon'), may hold values from -6 to 6
Outputs:
- filtered: float32 [368, 1440, 1024], P('day', 'lon')
The draws below stay inside these ranges and needn't reach their ends.
All inputs are finite; a program needn't handle non-finite values.
Results may differ from the reference program's by a relative error of at most 0.0003.
Values may be sent and summed in bfloat16 or wider, within the bound.
No kernel may reach another device: no remote copies, remote signals or barrier semaphores. Data moves between devices by JAX's collectives and lax.ppermute only.
A program may use at most 192 MiB of HBM per device.

```python
import jax
import jax.numpy as jnp
from jax import lax

COLS = 1024
LON = 1440
DAYS = 368
DAY_HALF = 15
LON_HALF = 10


def levels(stream_key, extent, cuts, least, top_value):
    def one(position, shards_of):
        draws = jax.random.uniform(jax.random.fold_in(jax.random.fold_in(stream_key, 6), position), (shards_of,), jnp.float32, least / len(cuts), top_value / len(cuts))
        return jnp.repeat(jnp.exp(draws), extent[position] // shards_of).reshape((-1,) + (1,) * (len(extent) - position - 1))

    level = one(*cuts[0])
    for cut in cuts[1:]:
        level = level * one(*cut)
    return level


def centred(stream_key, dims, deviation, reach, shards=(), kind=jnp.bfloat16):
    drawn = jax.random.normal(stream_key, dims, jnp.float32) * deviation
    if len(shards) > 0:
        drawn = levels(stream_key, dims, shards, -0.22, 0.18) * drawn
    return jnp.clip(drawn, min=-reach, max=reach).astype(kind)


def setup_inputs(seed: int = 0) -> dict:
    key_list = jax.random.split(jax.random.key(seed), 2)
    field = centred(key_list[0], (DAYS, LON, COLS), 1.0, 6.0, ((0, 16), (1, 16)))
    return {"field": field}


def running(values, dim, half):
    count = values.shape[dim] - 2 * half
    total = jnp.cumsum(values, axis=dim)
    first = jnp.zeros_like(lax.slice_in_dim(total, 0, 1, axis=dim))
    total = jnp.concatenate([first, total], axis=dim)
    upper = lax.slice_in_dim(total, 2 * half + 1, 2 * half + 1 + count, axis=dim)
    lower = lax.slice_in_dim(total, 0, count, axis=dim)
    return (upper - lower) / (2.0 * half + 1.0)


def wrapped(values, dim, half):
    size = values.shape[dim]
    head = lax.slice_in_dim(values, size - half, size, axis=dim)
    tail = lax.slice_in_dim(values, 0, half, axis=dim)
    return jnp.concatenate([head, values, tail], axis=dim)


def one_block(block):
    values = block.astype(jnp.float32)
    clim = running(wrapped(values, 0, DAY_HALF), 0, DAY_HALF)
    anomaly = values - clim
    return running(wrapped(anomaly, 1, LON_HALF), 1, LON_HALF)


def reference(field):
    width = 128 if COLS % 128 == 0 else COLS
    blocks = COLS // width
    split = field.reshape(DAYS, LON, blocks, width)
    split = jnp.moveaxis(split, 2, 0)
    result = lax.map(one_block, split)
    return jnp.moveaxis(result, 0, 2).reshape(DAYS, LON, COLS)
```

```python
import functools

import jax
import jax.numpy as jnp
from jax import lax
from jax.experimental import pallas as pl
from jax.experimental.pallas import tpu as pltpu
from jax.sharding import PartitionSpec as P

DAY_HALF = 15
LON_HALF = 10
DAY_PAD = 16
DAY_WIN = 2 * DAY_HALF + 1
LON_WIN = 2 * LON_HALF + 1
SCALE = 1.0 / (DAY_WIN * LON_WIN)
BLOCK = 256
WIDTHS = (256, 256, 256, 256)
VMEM = pl.BlockSpec(memory_space=pltpu.VMEM)


def day_matrices(days):
    def part(count, first):
        d = lax.broadcasted_iota(jnp.int32, (days, count), 0)
        s = lax.broadcasted_iota(jnp.int32, (days, count), 1) + first
        near = (s - d <= DAY_HALF) & (d - s <= DAY_HALF)
        return (jnp.where(s == d, float(DAY_WIN), 0.0) - jnp.where(near, 1.0, 0.0)).astype(jnp.bfloat16)

    return part(DAY_HALF, -DAY_HALF), part(days, 0), part(DAY_HALF, days)


def dot(a, b):
    return jnp.dot(a, b, preferred_element_type=jnp.float32)


def pack_kernel(groups, start, own, fwd, bwd):
    days, width = own.shape[1], fwd.shape[2]
    cols = slice(start, start + width)
    to = 0
    for first, count in groups:
        at, to = slice(to, to + count), to + count
        src = slice(first, first + count)
        fwd[at, :DAY_HALF, :] = own[src, days - DAY_HALF : days, cols]
        bwd[at, :DAY_HALF, :] = own[src, :DAY_HALF, cols]


def edge_kernel(field, left, right, to_right, to_left):
    lons, days, width = field.shape
    high = lons - LON_HALF
    ml, mo, mr = day_matrices(days)
    for c in range(width // BLOCK):
        cols = slice(c * BLOCK, (c + 1) * BLOCK)

        def anomaly(i):
            own = field[i if i < LON_HALF else high + i - LON_HALF, :, cols]
            halo_l = left[i, :DAY_HALF, cols]
            halo_r = right[i, :DAY_HALF, cols]
            return dot(ml, halo_l) + dot(mo, own) + dot(mr, halo_r)

        total = anomaly(0)
        to_left[0, :, cols] = total
        for j in range(1, LON_HALF):
            total = total + anomaly(j)
            to_left[j, :, cols] = total
        total = anomaly(2 * LON_HALF - 1)
        to_right[LON_HALF - 1, :, cols] = total
        for j in range(LON_HALF - 2, -1, -1):
            total = total + anomaly(LON_HALF + j)
            to_right[j, :, cols] = total


def main_kernel(start, own, edge_l, edge_r, mid_l, mid_r, from_l, from_r, prev, out, g):
    lons, days, _ = own.shape
    width = out.shape[2]
    high = lons - LON_HALF
    cols = slice(start, start + width)
    ml, mo, mr = day_matrices(days)

    def anomaly(l, left, right):
        g[l] = dot(ml, left) + dot(mo, own[l, :, cols]) + dot(mr, right)

    for l in range(LON_HALF):
        for at, e in ((l, l), (high + l, LON_HALF + l)):
            anomaly(at, edge_l[e, :DAY_HALF, cols], edge_r[e, :DAY_HALF, cols])

    def inner(i, _):
        anomaly(LON_HALF + i, mid_l[i, :DAY_HALF, :], mid_r[i, :DAY_HALF, :])
        return 0

    lax.fori_loop(0, high - LON_HALF, inner, 0, unroll=10)

    total = g[0]
    for l in range(1, LON_HALF):
        total = total + g[l]

    def first(l, total):
        total = total + g[l + LON_HALF]
        out[l] = (total + from_l[l, :, cols]) * SCALE
        return total

    def center(l, total):
        total = total + (g[l + LON_HALF] - g[l - LON_HALF - 1])
        out[l] = total * SCALE
        return total

    def last(l, total):
        total = total - g[l - LON_HALF - 1]
        out[l] = (total + from_r[l - high, :, cols]) * SCALE
        return total

    total = lax.fori_loop(0, LON_HALF, first, total, unroll=True)
    total = total + g[2 * LON_HALF]
    out[LON_HALF] = total * SCALE
    total = lax.fori_loop(LON_HALF + 1, high, center, total, unroll=3)
    lax.fori_loop(high, lons, last, total, unroll=True)


def local(field):
    field = jnp.transpose(field, (1, 0, 2))
    lons, days, cols = field.shape
    high = lons - LON_HALF
    mid = high - LON_HALF
    nday, nlon = lax.axis_size("day"), lax.axis_size("lon")
    params = pltpu.CompilerParams(vmem_limit_bytes=24 * 2**20)
    starts = [sum(WIDTHS[:c]) for c in range(len(WIDTHS))]

    def cost(work):
        return pl.CostEstimate(flops=10**3 * work, bytes_accessed=10 * work, transcendentals=0)

    def shift(x, axis, n, step):
        return lax.ppermute(x, axis, [(i, (i + step) % n) for i in range(n)])

    def halos(packed):
        fwd, bwd = packed
        return shift(fwd, "day", nday, 1), shift(bwd, "day", nday, -1)

    def pack(groups, start, width):
        shape = (sum(n for _, n in groups), DAY_PAD, width)
        packed = pl.pallas_call(
            functools.partial(pack_kernel, groups, start),
            in_specs=[VMEM],
            out_specs=[VMEM] * 2,
            out_shape=[jax.ShapeDtypeStruct(shape, field.dtype)] * 2,
            cost_estimate=cost(1000),
            compiler_params=params,
        )(field)
        return halos(packed)

    edge_l, edge_r = pack(((0, LON_HALF), (high, LON_HALF)), 0, cols)
    mids = [pack(((LON_HALF, mid),), starts[c], w) for c, w in enumerate(WIDTHS)]

    to_right, to_left = pl.pallas_call(
        edge_kernel,
        in_specs=[VMEM] * 3,
        out_specs=[VMEM] * 2,
        out_shape=[jax.ShapeDtypeStruct((LON_HALF, days, cols), jnp.float32)] * 2,
        cost_estimate=cost(5000),
        compiler_params=params,
        name="edge",
    )(field, edge_l, edge_r)
    from_l = shift(to_right, "lon", nlon, 1)
    from_r = shift(to_left, "lon", nlon, -1)

    out = None
    for c, width in enumerate(WIDTHS):
        at = pl.BlockSpec((lons, days, width), lambda i, c=c: (0, 0, starts[c] // WIDTHS[c]))
        specs = [VMEM] * 7
        args = [field, edge_l, edge_r, *mids[c], from_l, from_r]
        body = functools.partial(main_kernel, starts[c])
        if c:
            specs.append(pl.BlockSpec(memory_space=pl.ANY))
            args.append(out)
            fn, alias = body, {7: 0}
        else:
            fn, alias = lambda *refs, body=body: body(*refs[:7], None, *refs[7:]), {}
        out = pl.pallas_call(
            fn,
            grid=(1,),
            in_specs=specs,
            out_specs=at,
            out_shape=jax.ShapeDtypeStruct(field.shape, jnp.float32),
            input_output_aliases=alias,
            scratch_shapes=[pltpu.VMEM((lons, days, width), jnp.float32)],
            cost_estimate=cost(5000),
            compiler_params=params,
        )(*args)
    return jnp.transpose(out, (1, 0, 2))


def solution(mesh):
    return jax.shard_map(
        local,
        mesh=mesh,
        in_specs=(P("day", "lon", None),),
        out_specs=P("day", "lon", None),
        check_vma=False,
    )
```

```python
import functools

import jax
import jax.numpy as jnp
from jax import lax
from jax.experimental import pallas as pl
from jax.experimental.pallas import tpu as pltpu
from jax.sharding import PartitionSpec as P

DAY_HALF = 15
LON_HALF = 10
DAY_PAD = 16
DAY_WIN = 2 * DAY_HALF + 1
LON_WIN = 2 * LON_HALF + 1
SCALE = 1.0 / (DAY_WIN * LON_WIN)
BLOCK = 256
WIDTHS = (512, 256, 256)
PARTS = 2
VMEM = pl.BlockSpec(memory_space=pltpu.VMEM)
ANY = pl.BlockSpec(memory_space=pl.ANY)


def day_matrix(days, core):
    shape = (days, 2 * DAY_PAD + days)
    d = lax.broadcasted_iota(jnp.int32, shape, 0)
    col = lax.broadcasted_iota(jnp.int32, shape, 1)
    halo = col < 2 * DAY_PAD
    row = col % DAY_PAD
    from_left = (col < DAY_PAD) == (core == 0)
    s = jnp.where(halo, jnp.where(from_left, row - DAY_HALF, row + days), col - 2 * DAY_PAD)
    near = (s - d <= DAY_HALF) & (d - s <= DAY_HALF) & ((row < DAY_HALF) | ~halo)
    same = (s == d) & ~halo
    return (jnp.where(same, float(DAY_WIN), 0.0) - jnp.where(near, 1.0, 0.0)).astype(jnp.bfloat16)


def dot(a, *parts):
    return jnp.dot(a, jnp.concatenate(parts, axis=0), preferred_element_type=jnp.float32)


def is_direct(day):
    return (day % 4 == 1) | (day % 4 == 2)


def pack_kernel(groups, start, own, off, on):
    core = lax.axis_index("day") % 2
    days, width = own.shape[1], off.shape[2]
    cols = slice(start, start + width)

    def copy(late_days, early_days):
        late_days[...] = jnp.zeros_like(late_days)
        to = 0
        for first, count in groups:
            at, to = slice(to, to + count), to + count
            src = slice(first, first + count)
            late_days[at, :DAY_HALF, :] = own[src, days - DAY_HALF : days, cols]
            early_days[at, :, :] = own[src, :DAY_PAD, cols]

    @pl.when(core == 1)
    def _():
        copy(off, on)

    @pl.when(core == 0)
    def _():
        copy(on, off)


def edge_kernel(planes, field, off, on, to_right, to_left, first, second, either):
    lons, days, width = field.shape
    high = lons - LON_HALF
    day, z = lax.axis_index("day"), lax.axis_index("lon") % planes
    mat = day_matrix(days, day % 2)
    for c in range(width // BLOCK):
        cols = slice(c * BLOCK, (c + 1) * BLOCK)

        def anomaly(i):
            own = field[i if i < LON_HALF else high + i - LON_HALF, :, cols]
            return dot(mat, off[i, :, cols], on[i, :, cols], own)

        total = anomaly(0)
        to_left[0, :, cols] = total
        for j in range(1, LON_HALF):
            total = total + anomaly(j)
            to_left[j, :, cols] = total
        total = anomaly(2 * LON_HALF - 1)
        to_right[LON_HALF - 1, :, cols] = total
        for j in range(LON_HALF - 2, -1, -1):
            total = total + anomaly(LON_HALF + j)
            to_right[j, :, cols] = total

    half = width // 2

    def copy(src):
        first[...] = src[:, :, :half]
        second[...] = src[:, :, half:]

    @pl.when(z == 0)
    def _():
        copy(to_left)

    @pl.when(z != 0)
    def _():
        copy(to_right)

    either[...] = jnp.where(is_direct(day), second[...], first[...])


def main_kernel(start, own, edge_off, edge_on, mid_direct, mid_diag, mid_on, *rest):
    _, out, ends, g, buf, sems = rest
    lons, days, _ = own.shape
    width = mid_direct.shape[2]
    high = lons - LON_HALF
    day = lax.axis_index("day")
    mat = day_matrix(days, day % 2)
    direct = is_direct(day)
    step = (high - LON_HALF) // PARTS
    block = g.shape[2]

    def copies(b):
        cols = slice(start + b * block, start + (b + 1) * block)
        for k in range(PARTS):
            src = slice(k * step, (k + 1) * step)
            dst = slice(LON_HALF + k * step, LON_HALF + (k + 1) * step)
            yield pltpu.make_async_copy(buf.at[b % 2, src], out.at[dst, :, cols], sems.at[b % 2, k])

    blocks = width // block
    for b in range(blocks):
        first = start + b * block
        cols = slice(first, first + block)
        local_cols = slice(b * block, (b + 1) * block)

        for l in range(LON_HALF):
            for at, e in ((l, l), (high + l, LON_HALF + l)):
                g[at] = dot(mat, edge_off[e, :, cols], edge_on[e, :, cols], own[at, :, cols])

        def inner(i, _):
            l = LON_HALF + i
            off = jnp.where(direct, mid_direct[i, :, local_cols], mid_diag[i, :, cols])
            g[l] = dot(mat, off, mid_on[i, :, cols], own[l, :, cols])
            return 0

        lax.fori_loop(0, high - LON_HALF, inner, 0, unroll=10)
        if b >= 2:
            for copy in copies(b - 2):
                copy.wait()
        slot = buf.at[b % 2]
        moves = list(copies(b))

        total = g[0]
        for l in range(1, LON_HALF):
            total = total + g[l]
        for l in range(LON_HALF):
            total = total + g[l + LON_HALF]
            ends[l, :, local_cols] = total
        total = total + g[2 * LON_HALF]
        slot[0] = total * SCALE

        def center(l, total):
            total = total + (g[l + LON_HALF] - g[l - LON_HALF - 1])
            slot[l - LON_HALF] = total * SCALE
            return total

        at = LON_HALF + 1
        for k in range(PARTS):
            to = LON_HALF + (k + 1) * step
            total = lax.fori_loop(at, to, center, total, unroll=5)
            at = to
            moves[k].start()
        for j in range(LON_HALF):
            total = total - g[high + j - LON_HALF - 1]
            ends[LON_HALF + j, :, local_cols] = total
    for b in range(max(0, blocks - 2), blocks):
        for copy in copies(b):
            copy.wait()


def join_kernel(planes, starts, from_l, from_r, first, either, second, *rest):
    *ends, prev, out, buf, sems = rest
    high = out.shape[0] - LON_HALF
    day, z = lax.axis_index("day"), lax.axis_index("lon") % planes
    direct = is_direct(day)
    half = first.shape[2]
    moves = []
    for side, (near, plane, row) in enumerate(((from_l, 0, 0), (from_r, planes - 1, high))):
        gain = jnp.where(z == plane, 1.0, 0.0)
        for start, end in zip(starts, ends):
            for at in range(start, start + end.shape[2], BLOCK):
                cols = slice(at, at + BLOCK)
                own_cols = slice(at - start, at - start + BLOCK)
                a, b = (first, either) if at < half else (either, second)
                far_cols = slice(at % half, at % half + BLOCK)

                def add(j, _):
                    far = jnp.where(direct, a[j, :, far_cols], b[j, :, far_cols])
                    value = end[side * LON_HALF + j, :, own_cols] + near[j, :, cols] + far * gain
                    buf[side, j, :, cols] = value * SCALE
                    return 0

                lax.fori_loop(0, LON_HALF, add, 0, unroll=5)
        moves.append(pltpu.make_async_copy(buf.at[side], out.at[row : row + LON_HALF], sems.at[side]))
        moves[-1].start()
    for move in moves:
        move.wait()


def local(sizes, field):
    field = jnp.transpose(field, (1, 0, 2))
    lons, days, cols = field.shape
    high = lons - LON_HALF
    mid = high - LON_HALF
    nday, nlon = sizes
    nz = nlon // 2
    params = pltpu.CompilerParams(vmem_limit_bytes=24 * 2**20)
    starts = [sum(WIDTHS[:c]) for c in range(len(WIDTHS))]
    f32 = lambda w: jax.ShapeDtypeStruct((LON_HALF, days, w), jnp.float32)

    def cost(work):
        return pl.CostEstimate(flops=10**3 * work, bytes_accessed=10 * work, transcendentals=0)

    def swap(first, stride):
        pairs = []
        for i in range(first, nday, stride):
            pairs += [(i, (i + 1) % nday), ((i + 1) % nday, i)]
        return pairs

    def pack(groups, start, width):
        shape = (sum(n for _, n in groups), DAY_PAD, width)
        return pl.pallas_call(
            functools.partial(pack_kernel, groups, start),
            in_specs=[VMEM],
            out_specs=[VMEM] * 2,
            out_shape=[jax.ShapeDtypeStruct(shape, field.dtype)] * 2,
            cost_estimate=cost(1000),
            compiler_params=params,
        )(field)

    e_off, e_on = pack(((0, LON_HALF), (high, LON_HALF)), 0, cols)
    edge_off = lax.ppermute(e_off, "day", swap(1, 2))
    edge_on = lax.ppermute(e_on, "day", swap(0, 2))
    mid_direct = []
    for c, width in enumerate(WIDTHS):
        off, _ = pack(((LON_HALF, mid),), starts[c], width)
        mid_direct.append(lax.ppermute(off, "day", swap(1, 4)))
    off, on = pack(((LON_HALF, mid),), 0, cols)

    to_right, to_left, first, second, either = pl.pallas_call(
        functools.partial(edge_kernel, nz),
        in_specs=[VMEM] * 3,
        out_specs=[VMEM] * 5,
        out_shape=[f32(cols)] * 2 + [f32(cols // 2)] * 3,
        cost_estimate=cost(5000),
        compiler_params=params,
        name="edge",
    )(field, edge_off, edge_on)

    mid_on = lax.ppermute(on, "day", swap(0, 2))
    mid_diag = lax.ppermute(off, "day", swap(3, 4))

    at = lambda hi, zz, dd: (hi * nz + zz) * nday + dd
    last = nz - 1

    def via(planes, days_of):
        hop, land = [], []
        for hi in range(2):
            for dd in days_of:
                p = planes[dd % 4 in (1, 2)]
                for src, mid_z, dst in ((last, p, 0), (0, last - p, last)):
                    hop.append((at(hi, src, dd), at(hi, mid_z, dd ^ 3)))
                    land.append((at(hi, mid_z, dd ^ 3), at(1 - hi, dst, dd)))
        return hop, land

    all_days = range(nday)
    early = [dd for dd in all_days if dd % 4 in (0, 3)]
    late = [dd for dd in all_days if dd % 4 in (1, 2)]
    both_axes = ("lon", "day")
    hop_x, land_x = via({True: 1, False: 2}, all_days)
    hop_y, land_y = via({False: 3}, early)
    straight = []
    for hi in range(2):
        for dd in late:
            straight += [(at(hi, last, dd), at(1 - hi, 0, dd)), (at(hi, 0, dd), at(1 - hi, last, dd))]
    hopped_x = lax.ppermute(either, both_axes, hop_x)
    hopped_y = lax.ppermute(second, both_axes, hop_y)
    landed_0 = lax.ppermute(first, both_axes, straight)
    landed_x = lax.ppermute(hopped_x, both_axes, land_x)
    landed_y = lax.ppermute(hopped_y, both_axes, land_y)
    inner = [i for i in range(nlon) if i % nz != last]
    from_l = lax.ppermute(to_right, "lon", [(i, i + 1) for i in inner])
    from_r = lax.ppermute(to_left, "lon", [(i + 1, i) for i in inner])

    out, ends = None, []
    for c, width in enumerate(WIDTHS):
        args = [field, edge_off, edge_on, mid_direct[c], mid_diag, mid_on]
        specs = [VMEM] * len(args)
        body = functools.partial(main_kernel, starts[c])
        if c:
            specs.append(ANY)
            args.append(out)
            fn, alias = body, {len(args) - 1: 0}
        else:
            fn, alias = lambda *refs, body=body: body(*refs[:-5], None, *refs[-5:]), {}
        out, end = pl.pallas_call(
            fn,
            in_specs=specs,
            out_specs=[ANY, VMEM],
            out_shape=[
                jax.ShapeDtypeStruct(field.shape, jnp.float32),
                jax.ShapeDtypeStruct((2 * LON_HALF, days, width), jnp.float32),
            ],
            input_output_aliases=alias,
            scratch_shapes=[
                pltpu.VMEM((lons, days, BLOCK), jnp.float32),
                pltpu.VMEM((2, mid, days, BLOCK), jnp.float32),
                pltpu.SemaphoreType.DMA((2, PARTS)),
            ],
            cost_estimate=cost(5000),
            compiler_params=params,
        )(*args)
        ends.append(end)
    args = [from_l, from_r, landed_0, landed_x, landed_y, *ends, out]
    out = pl.pallas_call(
        functools.partial(join_kernel, nz, starts),
        in_specs=[VMEM] * (len(args) - 1) + [ANY],
        out_specs=ANY,
        out_shape=jax.ShapeDtypeStruct(field.shape, jnp.float32),
        input_output_aliases={len(args) - 1: 0},
        scratch_shapes=[
            pltpu.VMEM((2, LON_HALF, days, cols), jnp.float32),
            pltpu.SemaphoreType.DMA((2,)),
        ],
        cost_estimate=cost(3000),
        compiler_params=params,
        name="join",
    )(*args)
    return jnp.transpose(out, (1, 0, 2))


def solution(mesh):
    sizes = (mesh.shape["day"], mesh.shape["lon"])

    def body(field):
        return local(sizes, field)

    return jax.shard_map(
        body,
        mesh=mesh,
        in_specs=(P("day", "lon", None),),
        out_specs=P("day", "lon", None),
        check_vma=False,
    )
```

```python
import functools

import jax
import jax.numpy as jnp
from jax import lax
from jax.experimental import pallas as pl
from jax.experimental.pallas import tpu as pltpu
from jax.sharding import PartitionSpec as P

DAY_HALF = 15
LON_HALF = 10
DAY_PAD = 16
DAY_WIN = 2 * DAY_HALF + 1
LON_WIN = 2 * LON_HALF + 1
SCALE = 1.0 / (DAY_WIN * LON_WIN)
BLOCK = 256
WIDTHS = (512, 256, 128, 128)
AHEAD = 2
VMEM = pl.BlockSpec(memory_space=pltpu.VMEM)
ANY = pl.BlockSpec(memory_space=pl.ANY)


def window_weights(d, s, valid):
    return jnp.where((s - d <= DAY_HALF) & (d - s <= DAY_HALF) & valid, -1.0, 0.0)


def halo_day(row, days, from_left):
    return jnp.where(from_left, row - DAY_HALF, row + days)


def off_matrix(days, core):
    d = lax.broadcasted_iota(jnp.int32, (days, DAY_PAD), 0)
    row = lax.broadcasted_iota(jnp.int32, (days, DAY_PAD), 1)
    return window_weights(d, halo_day(row, days, core == 0), row < DAY_HALF).astype(jnp.bfloat16)


def spread_matrix(days, core):
    shape = (days, DAY_HALF * DAY_PAD)
    d = lax.broadcasted_iota(jnp.int32, shape, 0)
    col = lax.broadcasted_iota(jnp.int32, shape, 1)
    s = halo_day(col // DAY_PAD, days, core == 0)
    return window_weights(d, s, col % DAY_PAD == DAY_HALF).astype(jnp.bfloat16)


def rest_matrix(days, core):
    shape = (days, DAY_PAD + days)
    d = lax.broadcasted_iota(jnp.int32, shape, 0)
    col = lax.broadcasted_iota(jnp.int32, shape, 1)
    halo = col < DAY_PAD
    s = jnp.where(halo, halo_day(col, days, core == 1), col - DAY_PAD)
    same = jnp.where((s == d) & ~halo, float(DAY_WIN), 0.0)
    return (same + window_weights(d, s, ~halo | (col < DAY_HALF))).astype(jnp.bfloat16)


def dot(a, *parts):
    b = parts[0] if len(parts) == 1 else jnp.concatenate(parts, axis=0)
    return jnp.dot(a, b, preferred_element_type=jnp.float32)


def dense_tiles(lons):
    return -(-lons * DAY_HALF // DAY_PAD)


def is_direct(day):
    return (day % 4 == 1) | (day % 4 == 2)


def pack_dense(src, base, lons, low, cols, to):
    tiles = dense_tiles(lons)
    width = cols.stop - cols.start
    full = lons - tiles

    def rows(i):
        return src[base + i, low : low + DAY_HALF, cols].astype(jnp.float32)

    def store(i, last):
        to[i] = jnp.concatenate([rows(i), last], axis=0).astype(to.dtype)

    def group(q, _):
        extra = rows(tiles + q)
        for r in range(DAY_HALF):
            store(q * DAY_HALF + r, extra[r : r + 1])
        return 0

    lax.fori_loop(0, full, group, 0)
    for i in range(full * DAY_HALF, tiles):
        store(i, jnp.zeros((1, width), jnp.float32))


def pack_plain(src, base, lons, low, cols, to):
    width = cols.stop - cols.start

    def store(i, _):
        rows = src[base + i, low : low + DAY_HALF, cols].astype(jnp.float32)
        to[i] = jnp.concatenate([rows, jnp.zeros((1, width), jnp.float32)], axis=0).astype(to.dtype)
        return 0

    lax.fori_loop(0, lons, store, 0, unroll=5)


def by_core(core, days, run):
    @pl.when(core == 1)
    def _():
        run(days - DAY_HALF, 0)

    @pl.when(core == 0)
    def _():
        run(0, days - DAY_HALF)


def pack_edge_kernel(own, off, on):
    lons, days, width = own.shape
    cols = slice(0, width)

    def run(off_low, on_low):
        pack_dense(own, 0, lons, off_low, cols, off)
        pack_plain(own, 0, lons, on_low, cols, on)

    by_core(lax.axis_index("day") % 2, days, run)


def pack_off_kernel(start, wanted, own, off):
    lons, days, _ = own.shape
    day = lax.axis_index("day")
    cols = slice(start, start + off.shape[2])

    @pl.when(is_direct(day) == wanted)
    def _():
        def run(off_low, _):
            pack_dense(own, LON_HALF, lons - 2 * LON_HALF, off_low, cols, off)

        by_core(day % 2, days, run)


def pack_on_kernel(own, on):
    lons, days, width = own.shape

    def run(_, on_low):
        pack_plain(own, LON_HALF, lons - 2 * LON_HALF, on_low, slice(0, width), on)

    by_core(lax.axis_index("day") % 2, days, run)


def edge_part(days, core, off, cols):
    tiles = off.shape[0]
    tile_mat, spread_mat = off_matrix(days, core), spread_matrix(days, core)

    def part(i):
        if i < tiles:
            return dot(tile_mat, off[i, :, cols])
        first = (i - tiles) * DAY_HALF
        rows = off[first : first + DAY_HALF, :, cols]
        return dot(spread_mat, rows.reshape(DAY_HALF * DAY_PAD, rows.shape[2]))

    return part


def edge_kernel(planes, field, off, on, to_right, to_left, first, second):
    lons, days, width = field.shape
    high = lons - LON_HALF
    day, z = lax.axis_index("day"), lax.axis_index("lon") % planes
    mat = rest_matrix(days, day % 2)
    for c in range(width // BLOCK):
        cols = slice(c * BLOCK, (c + 1) * BLOCK)
        part = edge_part(days, day % 2, off, cols)

        def anomaly(i):
            own = field[i if i < LON_HALF else high + i - LON_HALF, :, cols]
            return dot(mat, on[i, :, cols], own) + part(i)

        total = anomaly(0)
        to_left[0, :, cols] = total
        for j in range(1, LON_HALF):
            total = total + anomaly(j)
            to_left[j, :, cols] = total
        total = anomaly(2 * LON_HALF - 1)
        to_right[LON_HALF - 1, :, cols] = total
        for j in range(LON_HALF - 2, -1, -1):
            total = total + anomaly(LON_HALF + j)
            to_right[j, :, cols] = total

    half = width // 2

    def copy(src):
        first[...] = src[:, :, :half]
        second[...] = src[:, :, half:]

    @pl.when(z == 0)
    def _():
        copy(to_left)

    @pl.when(z != 0)
    def _():
        copy(to_right)


def pre_kernel(field, edge_off, edge_on, mid_on, pre):
    lons, days, width = field.shape
    high = lons - LON_HALF
    core = lax.axis_index("day") % 2
    mat = rest_matrix(days, core)
    for c in range(width // BLOCK):
        cols = slice(c * BLOCK, (c + 1) * BLOCK)
        part = edge_part(days, core, edge_off, cols)
        for i in range(2 * LON_HALF):
            l = i if i < LON_HALF else high + i - LON_HALF
            pre[l, :, cols] = dot(mat, edge_on[i, :, cols], field[l, :, cols]) + part(i)

        def inner(i, _):
            l = LON_HALF + i
            pre[l, :, cols] = dot(mat, mid_on[i, :, cols], field[l, :, cols])
            return 0

        lax.fori_loop(0, high - LON_HALF, inner, 0, unroll=10)


def far_value(direct, far, j, start, width):
    half = far[0].shape[2]
    a, b = far[:2] if start < half else far[2:]
    cols = slice(start % half, start % half + width)
    return jnp.where(direct, a[j, :, cols], b[j, :, cols])


def main_kernel(planes, start, joined, pre, mid_direct, mid_diag, *rest):
    lon_args, moving = None, []
    if joined:
        lon_args, done, (prev, out, g, buf, sems, *spare) = rest[:6], rest[6 : 6 + len(joined)], rest[6 + len(joined) :]
        moving = start_join(planes, joined, lon_args, done, out, *spare)
    elif planes:
        *lon_args, prev, out, g, buf, sems = rest
    else:
        prev, out, ends, g, buf, sems = rest
    lons, days, _ = pre.shape
    width = mid_direct.shape[2]
    high = lons - LON_HALF
    mid = high - LON_HALF
    tiles = mid_direct.shape[0]
    day = lax.axis_index("day")
    direct = is_direct(day)
    tile_mat, spread_mat = off_matrix(days, day % 2), spread_matrix(days, day % 2)
    block = g.shape[2]
    base = (lons - buf.shape[1]) // 2
    parts = sems.shape[1]
    step = buf.shape[1] // parts
    if planes:
        z = lax.axis_index("lon") % planes
        gains = jnp.where(z == 0, 1.0, 0.0), jnp.where(z == planes - 1, 1.0, 0.0)

    def copies(b):
        cols = slice(start + b * block, start + (b + 1) * block)
        for k in range(parts):
            src = slice(k * step, (k + 1) * step)
            dst = slice(base + k * step, base + (k + 1) * step)
            yield pltpu.make_async_copy(buf.at[b % 2, src], out.at[dst, :, cols], sems.at[b % 2, k])

    blocks = width // block
    for b in range(blocks):
        first = start + b * block
        cols = slice(first, first + block)
        local_cols = slice(b * block, (b + 1) * block)

        for j in range(LON_HALF):
            g[j] = pre[j, :, cols]
            g[high + j] = pre[high + j, :, cols]

        def inner(i, _):
            off = jnp.where(direct, mid_direct[i, :, local_cols], mid_diag[i, :, cols])
            g[LON_HALF + i] = pre[LON_HALF + i, :, cols] + dot(tile_mat, off)
            return 0

        lax.fori_loop(0, tiles, inner, 0, unroll=11)
        for q in range(mid - tiles):
            at = slice(q * DAY_HALF, (q + 1) * DAY_HALF)
            off = jnp.where(direct, mid_direct[at, :, local_cols], mid_diag[at, :, cols])
            l = LON_HALF + tiles + q
            g[l] = pre[l, :, cols] + dot(spread_mat, off.reshape(DAY_HALF * DAY_PAD, block))
        if b >= 2:
            for copy in copies(b - 2):
                copy.wait()
        slot = buf.at[b % 2]
        moves = list(copies(b))

        def end(side, j, total):
            if not planes:
                ends[side * LON_HALF + j, :, local_cols] = total
                return
            near = lon_args[side][j, :, cols]
            far = far_value(direct, lon_args[2:], j, first, block)
            slot[(high if side else 0) + j] = (total + near + far * gains[side]) * SCALE

        total = g[0]
        for l in range(1, LON_HALF):
            total = total + g[l]
        for l in range(LON_HALF):
            total = total + g[l + LON_HALF]
            end(0, l, total)
        total = total + g[2 * LON_HALF]
        slot[LON_HALF - base] = total * SCALE

        def center(l, total):
            total = total + (g[l + LON_HALF] - g[l - LON_HALF - 1])
            slot[l - base] = total * SCALE
            return total

        at = LON_HALF + 1
        for k in range(parts):
            to = min(base + (k + 1) * step, high)
            total = lax.fori_loop(at, to, center, total, unroll=5)
            at = to
            if k < parts - 1 or not planes:
                moves[k].start()
        for j in range(LON_HALF):
            total = total - g[high + j - LON_HALF - 1]
            end(1, j, total)
        if planes:
            moves[-1].start()
    for b in range(max(0, blocks - 2), blocks):
        for copy in copies(b):
            copy.wait()
    for move in moving:
        move.wait()


def start_join(planes, starts, lon_args, ends, out, buf, sems):
    from_l, from_r, *far_args = lon_args
    width = buf.shape[3]
    high = out.shape[0] - LON_HALF
    day, z = lax.axis_index("day"), lax.axis_index("lon") % planes
    direct = is_direct(day)
    moves = []
    for side, (near, plane, row) in enumerate(((from_l, 0, 0), (from_r, planes - 1, high))):
        gain = jnp.where(z == plane, 1.0, 0.0)
        for start, end in zip(starts, ends):
            block = min(BLOCK, end.shape[2])
            for at in range(start, start + end.shape[2], block):
                cols = slice(at, at + block)
                own_cols = slice(at - start, at - start + block)

                def add(j, _):
                    far = far_value(direct, far_args, j, at, block)
                    value = end[side * LON_HALF + j, :, own_cols] + near[j, :, cols] + far * gain
                    buf[side, j, :, cols] = value * SCALE
                    return 0

                lax.fori_loop(0, LON_HALF, add, 0, unroll=5)
        moves.append(pltpu.make_async_copy(buf.at[side], out.at[row : row + LON_HALF, :, :width], sems.at[side]))
        moves[-1].start()
    return moves


def local(sizes, field):
    field = jnp.transpose(field, (1, 0, 2))
    lons, days, cols = field.shape
    mid = lons - 2 * LON_HALF
    nday, nlon = sizes
    nz = nlon // 2
    params = pltpu.CompilerParams(vmem_limit_bytes=12 * 2**20)
    starts = [sum(WIDTHS[:c]) for c in range(len(WIDTHS))]
    f32 = lambda w: jax.ShapeDtypeStruct((LON_HALF, days, w), jnp.float32)
    bf16 = lambda *shape: jax.ShapeDtypeStruct(shape, field.dtype)

    def cost(work):
        return pl.CostEstimate(flops=10**3 * work, bytes_accessed=10 * work, transcendentals=0)

    def swap(first, stride):
        pairs = []
        for i in range(first, nday, stride):
            pairs += [(i, (i + 1) % nday), ((i + 1) % nday, i)]
        return pairs

    def call(body, args, out, work=1000):
        return pl.pallas_call(
            body,
            in_specs=[VMEM] * len(args),
            out_specs=[VMEM] * len(out) if isinstance(out, list) else VMEM,
            out_shape=out,
            cost_estimate=cost(work),
            compiler_params=params,
        )(*args)

    ends_own = jnp.concatenate([field[:LON_HALF], field[lons - LON_HALF :]], axis=0)
    shapes = [bf16(dense_tiles(2 * LON_HALF), DAY_PAD, cols), bf16(2 * LON_HALF, DAY_PAD, cols)]
    e_off, e_on = call(pack_edge_kernel, [ends_own], shapes)
    edge_off = lax.ppermute(e_off, "day", swap(1, 2))
    edge_on = lax.ppermute(e_on, "day", swap(0, 2))

    mid_direct = []
    for c, width in enumerate(WIDTHS):
        off = call(functools.partial(pack_off_kernel, starts[c], True), [field], bf16(dense_tiles(mid), DAY_PAD, width))
        mid_direct.append(lax.ppermute(off, "day", swap(1, 4)))
    on = call(pack_on_kernel, [field], bf16(mid, DAY_PAD, cols))
    off = call(functools.partial(pack_off_kernel, 0, False), [field], bf16(dense_tiles(mid), DAY_PAD, cols))

    to_right, to_left, first, second = pl.pallas_call(
        functools.partial(edge_kernel, nz),
        in_specs=[VMEM] * 3,
        out_specs=[VMEM] * 4,
        out_shape=[f32(cols)] * 2 + [f32(cols // 2)] * 2,
        cost_estimate=cost(5000),
        compiler_params=params,
        name="edge",
    )(field, edge_off, edge_on)

    mid_on = lax.ppermute(on, "day", swap(0, 2))
    mid_diag = lax.ppermute(off, "day", swap(3, 4))

    at = lambda hi, zz, dd: (hi * nz + zz) * nday + dd
    last = nz - 1

    def via(p, days_of):
        hop, land = [], []
        for hi in range(2):
            for dd in days_of:
                for src, mid_z, dst in ((last, p, 0), (0, last - p, last)):
                    hop.append((at(hi, src, dd), at(hi, mid_z, dd ^ 3)))
                    land.append((at(hi, mid_z, dd ^ 3), at(1 - hi, dst, dd)))
        return hop, land

    diag_days = [dd for dd in range(nday) if dd % 4 in (0, 3)]
    direct_days = [dd for dd in range(nday) if dd % 4 in (1, 2)]
    both_axes = ("lon", "day")
    straight = []
    for hi in range(2):
        for dd in direct_days:
            straight += [(at(hi, last, dd), at(1 - hi, 0, dd)), (at(hi, 0, dd), at(1 - hi, last, dd))]
    landed = []
    for x, p, days_of in ((first, 2, diag_days), (second, 1, direct_days), (second, 3, diag_days)):
        hop, land = via(p, days_of)
        hopped = lax.ppermute(x, both_axes, hop)
        landed.append(lax.ppermute(hopped, both_axes, land))
    landed.insert(0, lax.ppermute(first, both_axes, straight))
    inner = [i for i in range(nlon) if i % nz != last]
    from_l = lax.ppermute(to_right, "lon", [(i, i + 1) for i in inner])
    from_r = lax.ppermute(to_left, "lon", [(i + 1, i) for i in inner])

    pre = call(pre_kernel, [field, edge_off, edge_on, mid_on], jax.ShapeDtypeStruct(field.shape, jnp.float32), work=9000)
    lon_args = [from_l, from_r, *landed]
    whole = jax.ShapeDtypeStruct(field.shape, jnp.float32)
    out, ends = None, []
    for c, width in enumerate(WIDTHS):
        own_join = c >= AHEAD
        joined = starts[:AHEAD] if c == AHEAD else []
        block = min(BLOCK, width)
        args = [pre, mid_direct[c], mid_diag] + (lon_args if own_join else []) + (ends if joined else [])
        specs = [VMEM] * len(args)
        body = functools.partial(main_kernel, nz if own_join else 0, starts[c], joined)
        if c:
            specs.append(ANY)
            args.append(out)
            fn, alias = body, {len(args) - 1: 0}
        else:
            fn, alias = lambda *refs, body=body: body(*refs[:-5], None, *refs[-5:]), {}
        slots = min(2, width // block)
        scratch = [
            pltpu.VMEM((lons, days, block), jnp.float32),
            pltpu.VMEM((slots, lons if own_join else mid, days, block), jnp.float32),
            pltpu.SemaphoreType.DMA((slots, 3 if own_join else 2)),
        ]
        if joined:
            scratch += [pltpu.VMEM((2, LON_HALF, days, starts[c]), jnp.float32), pltpu.SemaphoreType.DMA((2,))]
        tail = jax.ShapeDtypeStruct((2 * LON_HALF, days, width), jnp.float32)
        res = pl.pallas_call(
            fn,
            in_specs=specs,
            out_specs=[ANY] if own_join else [ANY, VMEM],
            out_shape=[whole] if own_join else [whole, tail],
            input_output_aliases=alias,
            scratch_shapes=scratch,
            cost_estimate=cost(5000),
            compiler_params=params,
        )(*args)
        out = res[0]
        ends += res[1:]
    return jnp.transpose(out, (1, 0, 2))


def solution(mesh):
    sizes = (mesh.shape["day"], mesh.shape["lon"])

    def body(field):
        return local(sizes, field)

    return jax.shard_map(
        body,
        mesh=mesh,
        in_specs=(P("day", "lon", None),),
        out_specs=P("day", "lon", None),
        check_vma=False,
    )
```

```python
import functools

import jax
import jax.numpy as jnp
from jax import lax
from jax.experimental import pallas as pl
from jax.experimental.pallas import tpu as pltpu
from jax.sharding import PartitionSpec as P

DAY_HALF = 15
LON_HALF = 10
DAY_PAD = 16
DAY_WIN = 2 * DAY_HALF + 1
LON_WIN = 2 * LON_HALF + 1
SCALE = 1.0 / (DAY_WIN * LON_WIN)
BLOCK = 256
WIDTHS = (512, 256, 128, 128)
JOINS = {2: (0,), 3: (1, 2)}
VMEM = pl.BlockSpec(memory_space=pltpu.VMEM)
ANY = pl.BlockSpec(memory_space=pl.ANY)


def window_weights(d, s, valid):
    return jnp.where((s - d <= DAY_HALF) & (d - s <= DAY_HALF) & valid, -1.0, 0.0)


def halo_day(row, days, from_left):
    return jnp.where(from_left, row - DAY_HALF, row + days)


def off_matrix(days, core):
    d = lax.broadcasted_iota(jnp.int32, (days, DAY_PAD), 0)
    row = lax.broadcasted_iota(jnp.int32, (days, DAY_PAD), 1)
    return window_weights(d, halo_day(row, days, core == 0), row < DAY_HALF).astype(jnp.bfloat16)


def spread_matrix(days, core):
    shape = (days, DAY_HALF * DAY_PAD)
    d = lax.broadcasted_iota(jnp.int32, shape, 0)
    col = lax.broadcasted_iota(jnp.int32, shape, 1)
    s = halo_day(col // DAY_PAD, days, core == 0)
    return window_weights(d, s, col % DAY_PAD == DAY_HALF).astype(jnp.bfloat16)


def rest_matrix(days, core):
    shape = (days, DAY_PAD + days)
    d = lax.broadcasted_iota(jnp.int32, shape, 0)
    col = lax.broadcasted_iota(jnp.int32, shape, 1)
    halo = col < DAY_PAD
    s = jnp.where(halo, halo_day(col, days, core == 1), col - DAY_PAD)
    same = jnp.where((s == d) & ~halo, float(DAY_WIN), 0.0)
    return (same + window_weights(d, s, ~halo | (col < DAY_HALF))).astype(jnp.bfloat16)


def dot(a, *parts):
    b = parts[0] if len(parts) == 1 else jnp.concatenate(parts, axis=0)
    return jnp.dot(a, b, preferred_element_type=jnp.float32)


def dense_tiles(lons):
    return -(-lons * DAY_HALF // DAY_PAD)


def is_direct(day):
    return (day % 4 == 1) | (day % 4 == 2)


def pack_dense(src, base, lons, low, cols, to):
    tiles = dense_tiles(lons)
    width = cols.stop - cols.start
    full = lons - tiles

    def rows(i):
        return src[base + i, low : low + DAY_HALF, cols].astype(jnp.float32)

    def store(i, last):
        to[i] = jnp.concatenate([rows(i), last], axis=0).astype(to.dtype)

    def group(q, _):
        extra = rows(tiles + q)
        for r in range(DAY_HALF):
            store(q * DAY_HALF + r, extra[r : r + 1])
        return 0

    lax.fori_loop(0, full, group, 0)
    for i in range(full * DAY_HALF, tiles):
        store(i, jnp.zeros((1, width), jnp.float32))


def pack_plain(src, base, lons, low, cols, to):
    width = cols.stop - cols.start

    def store(i, _):
        rows = src[base + i, low : low + DAY_HALF, cols].astype(jnp.float32)
        to[i] = jnp.concatenate([rows, jnp.zeros((1, width), jnp.float32)], axis=0).astype(to.dtype)
        return 0

    lax.fori_loop(0, lons, store, 0, unroll=5)


def by_core(core, days, run):
    @pl.when(core == 1)
    def _():
        run(days - DAY_HALF, 0)

    @pl.when(core == 0)
    def _():
        run(0, days - DAY_HALF)


def pack_edge_kernel(own, off, on):
    lons, days, width = own.shape
    cols = slice(0, width)

    def run(off_low, on_low):
        pack_dense(own, 0, lons, off_low, cols, off)
        pack_plain(own, 0, lons, on_low, cols, on)

    by_core(lax.axis_index("day") % 2, days, run)


def pack_off_kernel(start, wanted, own, off):
    lons, days, _ = own.shape
    day = lax.axis_index("day")
    cols = slice(start, start + off.shape[2])

    @pl.when(is_direct(day) == wanted)
    def _():
        def run(off_low, _):
            pack_dense(own, LON_HALF, lons - 2 * LON_HALF, off_low, cols, off)

        by_core(day % 2, days, run)


def pack_on_kernel(own, on):
    lons, days, width = own.shape

    def run(_, on_low):
        pack_plain(own, LON_HALF, lons - 2 * LON_HALF, on_low, slice(0, width), on)

    by_core(lax.axis_index("day") % 2, days, run)


def edge_part(days, core, off, cols):
    tiles = off.shape[0]
    tile_mat, spread_mat = off_matrix(days, core), spread_matrix(days, core)

    def part(i):
        if i < tiles:
            return dot(tile_mat, off[i, :, cols])
        first = (i - tiles) * DAY_HALF
        rows = off[first : first + DAY_HALF, :, cols]
        return dot(spread_mat, rows.reshape(DAY_HALF * DAY_PAD, rows.shape[2]))

    return part


def edge_kernel(planes, field, off, on, to_right, to_left, first, second):
    lons, days, width = field.shape
    high = lons - LON_HALF
    day, z = lax.axis_index("day"), lax.axis_index("lon") % planes
    mat = rest_matrix(days, day % 2)
    for c in range(width // BLOCK):
        cols = slice(c * BLOCK, (c + 1) * BLOCK)
        part = edge_part(days, day % 2, off, cols)

        def anomaly(i):
            own = field[i if i < LON_HALF else high + i - LON_HALF, :, cols]
            return dot(mat, on[i, :, cols], own) + part(i)

        total = anomaly(0)
        to_left[0, :, cols] = total
        for j in range(1, LON_HALF):
            total = total + anomaly(j)
            to_left[j, :, cols] = total
        total = anomaly(2 * LON_HALF - 1)
        to_right[LON_HALF - 1, :, cols] = total
        for j in range(LON_HALF - 2, -1, -1):
            total = total + anomaly(LON_HALF + j)
            to_right[j, :, cols] = total

    half = width // 2

    def copy(src):
        first[...] = src[:, :, :half]
        second[...] = src[:, :, half:]

    @pl.when(z == 0)
    def _():
        copy(to_left)

    @pl.when(z != 0)
    def _():
        copy(to_right)


def pre_kernel(field, edge_off, edge_on, mid_on, pre):
    lons, days, width = field.shape
    high = lons - LON_HALF
    core = lax.axis_index("day") % 2
    mat = rest_matrix(days, core)
    for c in range(width // BLOCK):
        cols = slice(c * BLOCK, (c + 1) * BLOCK)
        part = edge_part(days, core, edge_off, cols)
        for i in range(2 * LON_HALF):
            l = i if i < LON_HALF else high + i - LON_HALF
            pre[l, :, cols] = dot(mat, edge_on[i, :, cols], field[l, :, cols]) + part(i)

        def inner(i, _):
            l = LON_HALF + i
            pre[l, :, cols] = dot(mat, mid_on[i, :, cols], field[l, :, cols])
            return 0

        lax.fori_loop(0, high - LON_HALF, inner, 0, unroll=10)


def far_value(direct, far, j, start, width):
    half = far[0].shape[2]
    a, b = far[:2] if start < half else far[2:]
    cols = slice(start % half, start % half + width)
    return jnp.where(direct, a[j, :, cols], b[j, :, cols])


def main_kernel(planes, start, own_join, joined, lon_count, pre, mid_direct, mid_diag, *rest):
    lon_args, rest = rest[:lon_count], rest[lon_count:]
    done, rest = rest[: len(joined)], rest[len(joined) :]
    if own_join:
        prev, out, g, buf, sems, *spare = rest
    else:
        prev, out, ends, g, buf, sems, *spare = rest
    moving = start_join(planes, joined, lon_args, done, out, *spare) if joined else []
    lons, days, _ = pre.shape
    width = mid_direct.shape[2]
    high = lons - LON_HALF
    mid = high - LON_HALF
    tiles = mid_direct.shape[0]
    day = lax.axis_index("day")
    direct = is_direct(day)
    tile_mat, spread_mat = off_matrix(days, day % 2), spread_matrix(days, day % 2)
    block = g.shape[2]
    base = (lons - buf.shape[1]) // 2
    parts = sems.shape[1]
    step = buf.shape[1] // parts
    if own_join:
        z = lax.axis_index("lon") % planes
        gains = jnp.where(z == 0, 1.0, 0.0), jnp.where(z == planes - 1, 1.0, 0.0)

    def copies(b):
        cols = slice(start + b * block, start + (b + 1) * block)
        for k in range(parts):
            src = slice(k * step, (k + 1) * step)
            dst = slice(base + k * step, base + (k + 1) * step)
            yield pltpu.make_async_copy(buf.at[b % 2, src], out.at[dst, :, cols], sems.at[b % 2, k])

    blocks = width // block
    for b in range(blocks):
        first = start + b * block
        cols = slice(first, first + block)
        local_cols = slice(b * block, (b + 1) * block)

        for j in range(LON_HALF):
            g[j] = pre[j, :, cols]
            g[high + j] = pre[high + j, :, cols]

        def inner(i, _):
            off = jnp.where(direct, mid_direct[i, :, local_cols], mid_diag[i, :, cols])
            g[LON_HALF + i] = pre[LON_HALF + i, :, cols] + dot(tile_mat, off)
            return 0

        lax.fori_loop(0, tiles, inner, 0, unroll=True)
        for q in range(mid - tiles):
            at = slice(q * DAY_HALF, (q + 1) * DAY_HALF)
            off = jnp.where(direct, mid_direct[at, :, local_cols], mid_diag[at, :, cols])
            l = LON_HALF + tiles + q
            g[l] = pre[l, :, cols] + dot(spread_mat, off.reshape(DAY_HALF * DAY_PAD, block))
        if b >= 2:
            for copy in copies(b - 2):
                copy.wait()
        slot = buf.at[b % 2]
        moves = list(copies(b))

        def end(side, j, total):
            if not own_join:
                ends[side * LON_HALF + j, :, local_cols] = total
                return
            near = lon_args[side][j, :, cols]
            far = far_value(direct, lon_args[2:], j, first, block)
            slot[(high if side else 0) + j] = (total + near + far * gains[side]) * SCALE

        total = g[0]
        for l in range(1, LON_HALF):
            total = total + g[l]
        for l in range(LON_HALF):
            total = total + g[l + LON_HALF]
            end(0, l, total)
        total = total + g[2 * LON_HALF]
        slot[LON_HALF - base] = total * SCALE

        def center(l, total):
            total = total + (g[l + LON_HALF] - g[l - LON_HALF - 1])
            slot[l - base] = total * SCALE
            return total

        at = LON_HALF + 1
        for k in range(parts):
            to = min(base + (k + 1) * step, high)
            total = lax.fori_loop(at, to, center, total, unroll=True)
            at = to
            if k < parts - 1 or not own_join:
                moves[k].start()
        for j in range(LON_HALF):
            total = total - g[high + j - LON_HALF - 1]
            end(1, j, total)
        if own_join:
            moves[-1].start()
    for b in range(max(0, blocks - 2), blocks):
        for copy in copies(b):
            copy.wait()
    for move in moving:
        move.wait()


def start_join(planes, starts, lon_args, ends, out, buf, sems):
    from_l, from_r, *far_args = lon_args
    base, width = starts[0], buf.shape[3]
    high = out.shape[0] - LON_HALF
    day, z = lax.axis_index("day"), lax.axis_index("lon") % planes
    direct = is_direct(day)
    moves = []
    for side, (near, plane, row) in enumerate(((from_l, 0, 0), (from_r, planes - 1, high))):
        gain = jnp.where(z == plane, 1.0, 0.0)
        for start, end in zip(starts, ends):
            block = min(BLOCK, end.shape[2])
            for at in range(start, start + end.shape[2], block):
                cols = slice(at, at + block)
                own_cols = slice(at - start, at - start + block)

                def add(j, _):
                    far = far_value(direct, far_args, j, at, block)
                    value = end[side * LON_HALF + j, :, own_cols] + near[j, :, cols] + far * gain
                    buf[side, j, :, slice(at - base, at - base + block)] = value * SCALE
                    return 0

                lax.fori_loop(0, LON_HALF, add, 0, unroll=5)
        moves.append(pltpu.make_async_copy(buf.at[side], out.at[row : row + LON_HALF, :, base : base + width], sems.at[side]))
        moves[-1].start()
    return moves


def local(sizes, field):
    field = jnp.transpose(field, (1, 0, 2))
    lons, days, cols = field.shape
    mid = lons - 2 * LON_HALF
    nday, nlon = sizes
    nz = nlon // 2
    params = pltpu.CompilerParams(vmem_limit_bytes=12 * 2**20)
    starts = [sum(WIDTHS[:c]) for c in range(len(WIDTHS))]
    f32 = lambda w: jax.ShapeDtypeStruct((LON_HALF, days, w), jnp.float32)
    bf16 = lambda *shape: jax.ShapeDtypeStruct(shape, field.dtype)

    def cost(work):
        return pl.CostEstimate(flops=10**3 * work, bytes_accessed=10 * work, transcendentals=0)

    def swap(first, stride):
        pairs = []
        for i in range(first, nday, stride):
            pairs += [(i, (i + 1) % nday), ((i + 1) % nday, i)]
        return pairs

    def call(body, args, out, work=1000):
        return pl.pallas_call(
            body,
            in_specs=[VMEM] * len(args),
            out_specs=[VMEM] * len(out) if isinstance(out, list) else VMEM,
            out_shape=out,
            cost_estimate=cost(work),
            compiler_params=params,
        )(*args)

    ends_own = jnp.concatenate([field[:LON_HALF], field[lons - LON_HALF :]], axis=0)
    shapes = [bf16(dense_tiles(2 * LON_HALF), DAY_PAD, cols), bf16(2 * LON_HALF, DAY_PAD, cols)]
    e_off, e_on = call(pack_edge_kernel, [ends_own], shapes)
    edge_off = lax.ppermute(e_off, "day", swap(1, 2))
    edge_on = lax.ppermute(e_on, "day", swap(0, 2))

    mid_direct = []
    for c, width in enumerate(WIDTHS):
        off = call(functools.partial(pack_off_kernel, starts[c], True), [field], bf16(dense_tiles(mid), DAY_PAD, width))
        mid_direct.append(lax.ppermute(off, "day", swap(1, 4)))
    on = call(pack_on_kernel, [field], bf16(mid, DAY_PAD, cols))
    off = call(functools.partial(pack_off_kernel, 0, False), [field], bf16(dense_tiles(mid), DAY_PAD, cols))

    to_right, to_left, first, second = pl.pallas_call(
        functools.partial(edge_kernel, nz),
        in_specs=[VMEM] * 3,
        out_specs=[VMEM] * 4,
        out_shape=[f32(cols)] * 2 + [f32(cols // 2)] * 2,
        cost_estimate=cost(5000),
        compiler_params=params,
        name="edge",
    )(field, edge_off, edge_on)

    mid_on = lax.ppermute(on, "day", swap(0, 2))
    mid_diag = lax.ppermute(off, "day", swap(3, 4))

    at = lambda hi, zz, dd: (hi * nz + zz) * nday + dd
    last = nz - 1

    def via(p, days_of):
        hop, land = [], []
        for hi in range(2):
            for dd in days_of:
                for src, mid_z, dst in ((last, p, 0), (0, last - p, last)):
                    hop.append((at(hi, src, dd), at(hi, mid_z, dd ^ 3)))
                    land.append((at(hi, mid_z, dd ^ 3), at(1 - hi, dst, dd)))
        return hop, land

    diag_days = [dd for dd in range(nday) if dd % 4 in (0, 3)]
    direct_days = [dd for dd in range(nday) if dd % 4 in (1, 2)]
    both_axes = ("lon", "day")
    straight = []
    for hi in range(2):
        for dd in direct_days:
            straight += [(at(hi, last, dd), at(1 - hi, 0, dd)), (at(hi, 0, dd), at(1 - hi, last, dd))]
    landed = []
    for x, p, days_of in ((first, 2, diag_days), (second, 1, direct_days), (second, 3, diag_days)):
        hop, land = via(p, days_of)
        hopped = lax.ppermute(x, both_axes, hop)
        landed.append(lax.ppermute(hopped, both_axes, land))
    landed.insert(0, lax.ppermute(first, both_axes, straight))
    inner = [i for i in range(nlon) if i % nz != last]
    from_l = lax.ppermute(to_right, "lon", [(i, i + 1) for i in inner])
    from_r = lax.ppermute(to_left, "lon", [(i + 1, i) for i in inner])

    pre = call(pre_kernel, [field, edge_off, edge_on, mid_on], jax.ShapeDtypeStruct(field.shape, jnp.float32), work=9000)
    lon_args = [from_l, from_r, *landed]
    whole = jax.ShapeDtypeStruct(field.shape, jnp.float32)
    out, ends = None, []
    for c, width in enumerate(WIDTHS):
        joined = JOINS.get(c, ())
        own_join = c == len(WIDTHS) - 1
        needs = lon_args if own_join else lon_args[:4] if joined else []
        block = min(BLOCK, width)
        args = [pre, mid_direct[c], mid_diag, *needs, *(ends[k] for k in joined)]
        specs = [VMEM] * len(args)
        body = functools.partial(main_kernel, nz, starts[c], own_join, [starts[k] for k in joined], len(needs))
        if c:
            specs.append(ANY)
            args.append(out)
            fn, alias = body, {len(args) - 1: 0}
        else:
            fn, alias = lambda *refs, body=body: body(*refs[:-5], None, *refs[-5:]), {}
        slots = min(2, width // block)
        scratch = [
            pltpu.VMEM((lons, days, block), jnp.float32),
            pltpu.VMEM((slots, lons if own_join else mid, days, block), jnp.float32),
            pltpu.SemaphoreType.DMA((slots, 3 if own_join else 2)),
        ]
        if joined:
            scratch += [pltpu.VMEM((2, LON_HALF, days, sum(WIDTHS[k] for k in joined)), jnp.float32), pltpu.SemaphoreType.DMA((2,))]
        tail = jax.ShapeDtypeStruct((2 * LON_HALF, days, width), jnp.float32)
        res = pl.pallas_call(
            fn,
            in_specs=specs,
            out_specs=[ANY] if own_join else [ANY, VMEM],
            out_shape=[whole] if own_join else [whole, tail],
            input_output_aliases=alias,
            scratch_shapes=scratch,
            cost_estimate=cost(5000),
            compiler_params=params,
        )(*args)
        out = res[0]
        ends += res[1:]
    return jnp.transpose(out, (1, 0, 2))


def solution(mesh):
    sizes = (mesh.shape["day"], mesh.shape["lon"])

    def body(field):
        return local(sizes, field)

    return jax.shard_map(
        body,
        mesh=mesh,
        in_specs=(P("day", "lon", None),),
        out_specs=P("day", "lon", None),
        check_vma=False,
    )
```

```python
import functools

import jax
import jax.numpy as jnp
from jax import lax
from jax.experimental import pallas as pl
from jax.experimental.pallas import tpu as pltpu
from jax.sharding import PartitionSpec as P

DAY_HALF = 15
LON_HALF = 10
DAY_PAD = 16
DAY_WIN = 2 * DAY_HALF + 1
LON_WIN = 2 * LON_HALF + 1
SCALE = 1.0 / (DAY_WIN * LON_WIN)
BLOCK = 256
WIDTHS = (512, 256, 128, 128)
JOINS = {2: (0,), 3: (1, 2)}
VMEM = pl.BlockSpec(memory_space=pltpu.VMEM)
ANY = pl.BlockSpec(memory_space=pl.ANY)


def window_weights(d, s, valid):
    return jnp.where((s - d <= DAY_HALF) & (d - s <= DAY_HALF) & valid, -1.0, 0.0)


def halo_day(row, days, from_left):
    return jnp.where(from_left, row - DAY_HALF, row + days)


def off_matrix(days, core):
    d = lax.broadcasted_iota(jnp.int32, (days, DAY_PAD), 0)
    row = lax.broadcasted_iota(jnp.int32, (days, DAY_PAD), 1)
    return window_weights(d, halo_day(row, days, core == 0), row < DAY_HALF).astype(jnp.bfloat16)


def spread_matrix(days, core):
    shape = (days, DAY_HALF * DAY_PAD)
    d = lax.broadcasted_iota(jnp.int32, shape, 0)
    col = lax.broadcasted_iota(jnp.int32, shape, 1)
    s = halo_day(col // DAY_PAD, days, core == 0)
    return window_weights(d, s, col % DAY_PAD == DAY_HALF).astype(jnp.bfloat16)


def rest_matrix(days, core):
    shape = (days, DAY_PAD + days)
    d = lax.broadcasted_iota(jnp.int32, shape, 0)
    col = lax.broadcasted_iota(jnp.int32, shape, 1)
    halo = col < DAY_PAD
    s = jnp.where(halo, halo_day(col, days, core == 1), col - DAY_PAD)
    same = jnp.where((s == d) & ~halo, float(DAY_WIN), 0.0)
    return (same + window_weights(d, s, ~halo | (col < DAY_HALF))).astype(jnp.bfloat16)


def dot(a, *parts):
    b = parts[0] if len(parts) == 1 else jnp.concatenate(parts, axis=0)
    return jnp.dot(a, b, preferred_element_type=jnp.float32)


def dense_tiles(lons):
    return -(-lons * DAY_HALF // DAY_PAD)


def is_direct(day):
    return (day % 4 == 1) | (day % 4 == 2)


def pack_dense(src, base, lons, low, cols, to):
    tiles = dense_tiles(lons)
    width = cols.stop - cols.start
    full = lons - tiles

    def rows(i):
        return src[base + i, low : low + DAY_HALF, cols].astype(jnp.float32)

    def store(i, last):
        to[i] = jnp.concatenate([rows(i), last], axis=0).astype(to.dtype)

    def group(q, _):
        extra = rows(tiles + q)
        for r in range(DAY_HALF):
            store(q * DAY_HALF + r, extra[r : r + 1])
        return 0

    lax.fori_loop(0, full, group, 0)
    for i in range(full * DAY_HALF, tiles):
        store(i, jnp.zeros((1, width), jnp.float32))


def pack_plain(src, base, lons, low, cols, to):
    width = cols.stop - cols.start

    def store(i, _):
        rows = src[base + i, low : low + DAY_HALF, cols].astype(jnp.float32)
        to[i] = jnp.concatenate([rows, jnp.zeros((1, width), jnp.float32)], axis=0).astype(to.dtype)
        return 0

    lax.fori_loop(0, lons, store, 0, unroll=5)


def by_core(core, days, run):
    @pl.when(core == 1)
    def _():
        run(days - DAY_HALF, 0)

    @pl.when(core == 0)
    def _():
        run(0, days - DAY_HALF)


def pack_edge_kernel(field, off, on, own, sems):
    lons, days, width = field.shape
    moves = []
    for k, at in enumerate((0, lons - LON_HALF)):
        part = own.at[k * LON_HALF : (k + 1) * LON_HALF]
        moves.append(pltpu.make_async_copy(field.at[at : at + LON_HALF], part, sems.at[k]))
        moves[-1].start()
    for move in moves:
        move.wait()
    cols = slice(0, width)

    def run(off_low, on_low):
        pack_dense(own, 0, 2 * LON_HALF, off_low, cols, off)
        pack_plain(own, 0, 2 * LON_HALF, on_low, cols, on)

    by_core(lax.axis_index("day") % 2, days, run)


def pack_off_kernel(start, wanted, own, off):
    lons, days, _ = own.shape
    day = lax.axis_index("day")
    cols = slice(start, start + off.shape[2])

    @pl.when(is_direct(day) == wanted)
    def _():
        def run(off_low, _):
            pack_dense(own, LON_HALF, lons - 2 * LON_HALF, off_low, cols, off)

        by_core(day % 2, days, run)


def pack_on_kernel(own, on):
    lons, days, width = own.shape

    def run(_, on_low):
        pack_plain(own, LON_HALF, lons - 2 * LON_HALF, on_low, slice(0, width), on)

    by_core(lax.axis_index("day") % 2, days, run)


def edge_part(days, core, off, cols):
    tiles = off.shape[0]
    tile_mat, spread_mat = off_matrix(days, core), spread_matrix(days, core)

    def part(i):
        if i < tiles:
            return dot(tile_mat, off[i, :, cols])
        first = (i - tiles) * DAY_HALF
        rows = off[first : first + DAY_HALF, :, cols]
        return dot(spread_mat, rows.reshape(DAY_HALF * DAY_PAD, rows.shape[2]))

    return part


def edge_kernel(planes, field, off, on, to_right, to_left, first, second):
    lons, days, width = field.shape
    high = lons - LON_HALF
    day, z = lax.axis_index("day"), lax.axis_index("lon") % planes
    mat = rest_matrix(days, day % 2)
    for c in range(width // BLOCK):
        cols = slice(c * BLOCK, (c + 1) * BLOCK)
        part = edge_part(days, day % 2, off, cols)

        def anomaly(i):
            own = field[i if i < LON_HALF else high + i - LON_HALF, :, cols]
            return dot(mat, on[i, :, cols], own) + part(i)

        total = anomaly(0)
        to_left[0, :, cols] = total
        for j in range(1, LON_HALF):
            total = total + anomaly(j)
            to_left[j, :, cols] = total
        total = anomaly(2 * LON_HALF - 1)
        to_right[LON_HALF - 1, :, cols] = total
        for j in range(LON_HALF - 2, -1, -1):
            total = total + anomaly(LON_HALF + j)
            to_right[j, :, cols] = total

    half = width // 2

    def copy(src):
        first[...] = src[:, :, :half]
        second[...] = src[:, :, half:]

    @pl.when(z == 0)
    def _():
        copy(to_left)

    @pl.when(z != 0)
    def _():
        copy(to_right)


def pre_kernel(field, edge_off, edge_on, mid_on, pre):
    lons, days, width = field.shape
    high = lons - LON_HALF
    core = lax.axis_index("day") % 2
    mat = rest_matrix(days, core)
    for c in range(width // BLOCK):
        cols = slice(c * BLOCK, (c + 1) * BLOCK)
        part = edge_part(days, core, edge_off, cols)
        for i in range(2 * LON_HALF):
            l = i if i < LON_HALF else high + i - LON_HALF
            pre[l, :, cols] = dot(mat, edge_on[i, :, cols], field[l, :, cols]) + part(i)

        def inner(i, _):
            l = LON_HALF + i
            pre[l, :, cols] = dot(mat, mid_on[i, :, cols], field[l, :, cols])
            return 0

        lax.fori_loop(0, high - LON_HALF, inner, 0, unroll=10)


def far_value(direct, far, j, start, width):
    half = far[0].shape[2]
    a, b = far[:2] if start < half else far[2:]
    cols = slice(start % half, start % half + width)
    return jnp.where(direct, a[j, :, cols], b[j, :, cols])


def main_kernel(planes, start, own_join, joined, lon_count, pre, mid_direct, mid_diag, *rest):
    lon_args, rest = rest[:lon_count], rest[lon_count:]
    done, rest = rest[: len(joined)], rest[len(joined) :]
    if own_join:
        prev, out, g, buf, sems, *spare = rest
    else:
        prev, out, ends, g, buf, sems, *spare = rest
    moving = start_join(planes, joined, lon_args, done, out, *spare) if joined else []
    lons, days, _ = pre.shape
    width = mid_direct.shape[2]
    high = lons - LON_HALF
    mid = high - LON_HALF
    tiles = mid_direct.shape[0]
    day = lax.axis_index("day")
    direct = is_direct(day)
    tile_mat, spread_mat = off_matrix(days, day % 2), spread_matrix(days, day % 2)
    block = g.shape[2]
    base = (lons - buf.shape[1]) // 2
    parts = sems.shape[1]
    step = buf.shape[1] // parts
    if own_join:
        z = lax.axis_index("lon") % planes
        gains = jnp.where(z == 0, 1.0, 0.0), jnp.where(z == planes - 1, 1.0, 0.0)

    def copies(b):
        cols = slice(start + b * block, start + (b + 1) * block)
        for k in range(parts):
            src = slice(k * step, (k + 1) * step)
            dst = slice(base + k * step, base + (k + 1) * step)
            yield pltpu.make_async_copy(buf.at[b % 2, src], out.at[dst, :, cols], sems.at[b % 2, k])

    blocks = width // block
    for b in range(blocks):
        first = start + b * block
        cols = slice(first, first + block)
        local_cols = slice(b * block, (b + 1) * block)

        for j in range(LON_HALF):
            g[j] = pre[j, :, cols]
            g[high + j] = pre[high + j, :, cols]

        def inner(i, _):
            off = jnp.where(direct, mid_direct[i, :, local_cols], mid_diag[i, :, cols])
            g[LON_HALF + i] = pre[LON_HALF + i, :, cols] + dot(tile_mat, off)
            return 0

        lax.fori_loop(0, tiles, inner, 0, unroll=True)
        for q in range(mid - tiles):
            at = slice(q * DAY_HALF, (q + 1) * DAY_HALF)
            off = jnp.where(direct, mid_direct[at, :, local_cols], mid_diag[at, :, cols])
            l = LON_HALF + tiles + q
            g[l] = pre[l, :, cols] + dot(spread_mat, off.reshape(DAY_HALF * DAY_PAD, block))
        if b >= 2:
            for copy in copies(b - 2):
                copy.wait()
        slot = buf.at[b % 2]
        moves = list(copies(b))

        def end(side, j, total):
            if not own_join:
                ends[side * LON_HALF + j, :, local_cols] = total
                return
            near = lon_args[side][j, :, cols]
            far = far_value(direct, lon_args[2:], j, first, block)
            slot[(high if side else 0) + j] = (total + near + far * gains[side]) * SCALE

        total = g[0]
        for l in range(1, LON_HALF):
            total = total + g[l]
        for l in range(LON_HALF):
            total = total + g[l + LON_HALF]
            end(0, l, total)
        total = total + g[2 * LON_HALF]
        slot[LON_HALF - base] = total * SCALE

        def center(l, total):
            total = total + (g[l + LON_HALF] - g[l - LON_HALF - 1])
            slot[l - base] = total * SCALE
            return total

        at = LON_HALF + 1
        for k in range(parts):
            to = min(base + (k + 1) * step, high)
            total = lax.fori_loop(at, to, center, total, unroll=True)
            at = to
            if k < parts - 1 or not own_join:
                moves[k].start()
        for j in range(LON_HALF):
            total = total - g[high + j - LON_HALF - 1]
            end(1, j, total)
        if own_join:
            moves[-1].start()
    for b in range(max(0, blocks - 2), blocks):
        for copy in copies(b):
            copy.wait()
    for move in moving:
        move.wait()


def start_join(planes, starts, lon_args, ends, out, buf, sems):
    from_l, from_r, *far_args = lon_args
    base, width = starts[0], buf.shape[3]
    high = out.shape[0] - LON_HALF
    day, z = lax.axis_index("day"), lax.axis_index("lon") % planes
    direct = is_direct(day)
    moves = []
    for side, (near, plane, row) in enumerate(((from_l, 0, 0), (from_r, planes - 1, high))):
        gain = jnp.where(z == plane, 1.0, 0.0)
        for start, end in zip(starts, ends):
            block = min(BLOCK, end.shape[2])
            for at in range(start, start + end.shape[2], block):
                cols = slice(at, at + block)
                own_cols = slice(at - start, at - start + block)

                def add(j, _):
                    far = far_value(direct, far_args, j, at, block)
                    value = end[side * LON_HALF + j, :, own_cols] + near[j, :, cols] + far * gain
                    buf[side, j, :, slice(at - base, at - base + block)] = value * SCALE
                    return 0

                lax.fori_loop(0, LON_HALF, add, 0, unroll=True)
        moves.append(pltpu.make_async_copy(buf.at[side], out.at[row : row + LON_HALF, :, base : base + width], sems.at[side]))
        moves[-1].start()
    return moves


def local(sizes, field):
    field = jnp.transpose(field, (1, 0, 2))
    lons, days, cols = field.shape
    mid = lons - 2 * LON_HALF
    nday, nlon = sizes
    nz = nlon // 2
    params = pltpu.CompilerParams(vmem_limit_bytes=12 * 2**20)
    starts = [sum(WIDTHS[:c]) for c in range(len(WIDTHS))]
    f32 = lambda w: jax.ShapeDtypeStruct((LON_HALF, days, w), jnp.float32)
    bf16 = lambda *shape: jax.ShapeDtypeStruct(shape, field.dtype)

    def cost(work):
        return pl.CostEstimate(flops=10**3 * work, bytes_accessed=10 * work, transcendentals=0)

    def swap(first, stride):
        pairs = []
        for i in range(first, nday, stride):
            pairs += [(i, (i + 1) % nday), ((i + 1) % nday, i)]
        return pairs

    def call(body, args, out, work=1000):
        return pl.pallas_call(
            body,
            in_specs=[VMEM] * len(args),
            out_specs=[VMEM] * len(out) if isinstance(out, list) else VMEM,
            out_shape=out,
            cost_estimate=cost(work),
            compiler_params=params,
        )(*args)

    e_off, e_on = pl.pallas_call(
        pack_edge_kernel,
        in_specs=[ANY],
        out_specs=[VMEM] * 2,
        out_shape=[bf16(dense_tiles(2 * LON_HALF), DAY_PAD, cols), bf16(2 * LON_HALF, DAY_PAD, cols)],
        scratch_shapes=[pltpu.VMEM((2 * LON_HALF, days, cols), field.dtype), pltpu.SemaphoreType.DMA((2,))],
        cost_estimate=cost(1000),
        compiler_params=pltpu.CompilerParams(vmem_limit_bytes=52 * 2**20),
        name="packe",
    )(field)
    edge_off = lax.ppermute(e_off, "day", swap(1, 2))
    edge_on = lax.ppermute(e_on, "day", swap(0, 2))

    mid_direct = []
    for c, width in enumerate(WIDTHS):
        off = call(functools.partial(pack_off_kernel, starts[c], True), [field], bf16(dense_tiles(mid), DAY_PAD, width))
        mid_direct.append(lax.ppermute(off, "day", swap(1, 4)))
    on = call(pack_on_kernel, [field], bf16(mid, DAY_PAD, cols))
    off = call(functools.partial(pack_off_kernel, 0, False), [field], bf16(dense_tiles(mid), DAY_PAD, cols))

    to_right, to_left, first, second = pl.pallas_call(
        functools.partial(edge_kernel, nz),
        in_specs=[VMEM] * 3,
        out_specs=[VMEM] * 4,
        out_shape=[f32(cols)] * 2 + [f32(cols // 2)] * 2,
        cost_estimate=cost(5000),
        compiler_params=params,
        name="edge",
    )(field, edge_off, edge_on)

    mid_on = lax.ppermute(on, "day", swap(0, 2))
    mid_diag = lax.ppermute(off, "day", swap(3, 4))

    at = lambda hi, zz, dd: (hi * nz + zz) * nday + dd
    last = nz - 1

    def via(p, days_of):
        hop, land = [], []
        for hi in range(2):
            for dd in days_of:
                for src, mid_z, dst in ((last, p, 0), (0, last - p, last)):
                    hop.append((at(hi, src, dd), at(hi, mid_z, dd ^ 3)))
                    land.append((at(hi, mid_z, dd ^ 3), at(1 - hi, dst, dd)))
        return hop, land

    diag_days = [dd for dd in range(nday) if dd % 4 in (0, 3)]
    direct_days = [dd for dd in range(nday) if dd % 4 in (1, 2)]
    both_axes = ("lon", "day")
    straight = []
    for hi in range(2):
        for dd in direct_days:
            straight += [(at(hi, last, dd), at(1 - hi, 0, dd)), (at(hi, 0, dd), at(1 - hi, last, dd))]
    landed = []
    for x, p, days_of in ((first, 2, diag_days), (second, 1, direct_days), (second, 3, diag_days)):
        hop, land = via(p, days_of)
        hopped = lax.ppermute(x, both_axes, hop)
        landed.append(lax.ppermute(hopped, both_axes, land))
    landed.insert(0, lax.ppermute(first, both_axes, straight))
    inner = [i for i in range(nlon) if i % nz != last]
    from_l = lax.ppermute(to_right, "lon", [(i, i + 1) for i in inner])
    from_r = lax.ppermute(to_left, "lon", [(i + 1, i) for i in inner])

    pre = call(pre_kernel, [field, edge_off, edge_on, mid_on], jax.ShapeDtypeStruct(field.shape, jnp.float32), work=9000)
    lon_args = [from_l, from_r, *landed]
    whole = jax.ShapeDtypeStruct(field.shape, jnp.float32)
    out, ends = None, []
    for c, width in enumerate(WIDTHS):
        joined = JOINS.get(c, ())
        own_join = c == len(WIDTHS) - 1
        needs = lon_args if own_join else lon_args[:4] if joined else []
        block = min(BLOCK, width)
        args = [pre, mid_direct[c], mid_diag, *needs, *(ends[k] for k in joined)]
        specs = [VMEM] * len(args)
        body = functools.partial(main_kernel, nz, starts[c], own_join, [starts[k] for k in joined], len(needs))
        if c:
            specs.append(ANY)
            args.append(out)
            fn, alias = body, {len(args) - 1: 0}
        else:
            fn, alias = lambda *refs, body=body: body(*refs[:-5], None, *refs[-5:]), {}
        slots = min(2, width // block)
        scratch = [
            pltpu.VMEM((lons, days, block), jnp.float32),
            pltpu.VMEM((slots, lons if own_join else mid, days, block), jnp.float32),
            pltpu.SemaphoreType.DMA((slots, 5 if own_join else 2)),
        ]
        if joined:
            scratch += [pltpu.VMEM((2, LON_HALF, days, sum(WIDTHS[k] for k in joined)), jnp.float32), pltpu.SemaphoreType.DMA((2,))]
        tail = jax.ShapeDtypeStruct((2 * LON_HALF, days, width), jnp.float32)
        res = pl.pallas_call(
            fn,
            in_specs=specs,
            out_specs=[ANY] if own_join else [ANY, VMEM],
            out_shape=[whole] if own_join else [whole, tail],
            input_output_aliases=alias,
            scratch_shapes=scratch,
            cost_estimate=cost(5000),
            compiler_params=params,
        )(*args)
        out = res[0]
        ends += res[1:]
    return jnp.transpose(out, (1, 0, 2))


def solution(mesh):
    sizes = (mesh.shape["day"], mesh.shape["lon"])

    def body(field):
        return local(sizes, field)

    return jax.shard_map(
        body,
        mesh=mesh,
        in_specs=(P("day", "lon", None),),
        out_specs=P("day", "lon", None),
        check_vma=False,
    )
```
